128 devices in a mesh: seq: 16 (over z, x_hi, core), tp: 8 (over x_lo, y).
Axes of the slice: x: 4 (x_hi: 2, x_lo: 2; x = x_hi * 2 + x_lo), y: 4, z: 4, core: 2. Of those that a mesh axis runs over, the one named last changes fastest.
Arguments:
- tokens: bfloat16 [2, 3072, 4096], P(None, 'seq', 'tp'), may hold values from -6 to 6
- gate_weight: bfloat16 [4096, 4096], P(None, 'tp'), may hold values from -0.09375 to 0.09375
- cand_weight: bfloat16 [4096, 4096], P(None, 'tp'), may hold values from -0.09375 to 0.09375
- forget_bias: float32 [4096], P('tp'), may hold values from -1 to 9
- readout: bfloat16 [2, 3072, 4096], P(None, 'seq', 'tp'), may hold values from -6 to 6
- advantage: int32 [2, 3072], P(None, 'seq'), may hold values from -4 to 4
Outputs:
- grad_gate: float32 [4096, 4096], P('seq', 'tp')
- grad_cand: float32 [4096, 4096], P('seq', 'tp')
- grad_tokens: bfloat16 [2, 3072, 4096], P(None, 'seq', 'tp')
The draws below stay inside these ranges and needn't reach their ends.
All inputs are finite; a program needn't handle non-finite values.
Results may differ from the reference program's by a relative error of at most 0.014.
Values may be sent and summed in bfloat16 or wider, within the bound.
No kernel may reach another device: no remote copies, remote signals or barrier semaphores. Data moves between devices by JAX's collectives and lax.ppermute only.
A program may use at most 128 MiB of HBM per device.

```python
import jax
import jax.numpy as jnp
from jax import lax

D = 4096
H = 4096
SEQLEN = 3072


def plant(entries, stream_key, smallest, largest):
    longest = entries.shape.index(max(entries.shape))
    spots = []
    for shift in (0, 1):
        where = [jax.random.randint(jax.random.fold_in(stream_key, axis), (), 0, length) for axis, length in enumerate(entries.shape)]
        where[longest] = (where[longest] + shift) % entries.shape[longest]
        spots.append(tuple(where))
    return entries.at[spots[0]].set(smallest).at[spots[1]].set(largest)


def block_scale(own_key, shape, cuts, low, largest):
    def one(axis_at, shards_of):
        steps = jax.random.uniform(jax.random.fold_in(jax.random.fold_in(own_key, 6), axis_at), (shards_of,), jnp.float32, low / len(cuts), largest / len(cuts))
        return jnp.repeat(jnp.exp(steps), shape[axis_at] // shards_of).reshape((-1,) + (1,) * (len(shape) - axis_at - 1))

    level = one(*cuts[0])
    for cut in cuts[1:]:
        level = level * one(*cut)
    return level


def normal_values(stream_key, extent, deviation, most, pieces=(), held_as=jnp.bfloat16):
    values = jax.random.normal(stream_key, extent, jnp.float32) * deviation
    if len(pieces) > 0:
        values = block_scale(stream_key, extent, pieces, -0.22, 0.18) * values
    return jnp.clip(values, min=-most, max=most).astype(held_as)


def setup_inputs(seed: int = 0) -> dict:
    keys = jax.random.split(jax.random.key(seed), 7)
    tokens = normal_values(keys[0], (2, SEQLEN, D), 1.0, 6.0, ((1, 16), (2, 8)))
    gate_weight = normal_values(keys[1], (D, H), D ** -0.5, 0.09375, ((1, 8),))
    cand_weight = normal_values(keys[2], (D, H), D ** -0.5, 0.09375, ((1, 8),))
    forget_bias = jnp.clip(-1.0 + 10.0 * jax.random.uniform(keys[3], (H,), jnp.float32) ** block_scale(keys[3], (H,), ((0, 8),), -0.2, 0.2), -1.0, 9.0)
    readout = normal_values(keys[4], (2, SEQLEN, H), 1.0, 6.0, ((1, 16), (2, 8)))
    advantage = plant(jax.random.randint(keys[5], (2, SEQLEN), -4, 5), jax.random.fold_in(keys[5], 1), -4, 4).astype(jnp.int32)
    return {"tokens": tokens, "gate_weight": gate_weight, "cand_weight": cand_weight, "forget_bias": forget_bias, "readout": readout, "advantage": advantage}


def reference(tokens, gate_weight, cand_weight, forget_bias, readout, advantage):
    flat = tokens.reshape(-1, D)
    pre = jnp.dot(flat, gate_weight, preferred_element_type=jnp.float32).reshape(2, SEQLEN, H)
    cand = jnp.dot(flat, cand_weight, preferred_element_type=jnp.float32).reshape(2, SEQLEN, H)
    keep = jax.nn.sigmoid(pre + forget_bias.astype(jnp.float32))

    def forward(carry, inputs):
        kept, fresh = inputs
        carry = kept * carry + (1.0 - kept) * fresh
        return carry, carry

    start = jnp.zeros((2, H), jnp.float32)
    _, states = lax.scan(forward, start, (jnp.moveaxis(keep, 1, 0), jnp.moveaxis(cand, 1, 0)))
    state = jnp.moveaxis(states, 0, 1)
    prev = jnp.concatenate([jnp.zeros((2, 1, H), jnp.float32), state[:, :-1]], axis=1)
    score = (advantage.astype(jnp.float32) * 0.25)[:, :, None] * readout.astype(jnp.float32)
    coef = jnp.concatenate([keep[:, 1:], jnp.ones((2, 1, H), jnp.float32)], axis=1)

    def backward(carry, inputs):
        factor, term = inputs
        carry = term + factor * carry
        return carry, carry

    _, adjoints = lax.scan(backward, start, (jnp.moveaxis(coef, 1, 0), jnp.moveaxis(score, 1, 0)), reverse=True)
    adjoint = jnp.moveaxis(adjoints, 0, 1)
    dpre = (adjoint * (prev - cand) * keep * (1.0 - keep)).astype(jnp.bfloat16).reshape(-1, H)
    dcand = (adjoint * (1.0 - keep)).astype(jnp.bfloat16).reshape(-1, H)
    grad_gate = jnp.dot(flat.T, dpre, preferred_element_type=jnp.float32)
    grad_cand = jnp.dot(flat.T, dcand, preferred_element_type=jnp.float32)
    inputs_grad = jnp.dot(dpre, gate_weight.T, preferred_element_type=jnp.float32) + jnp.dot(dcand, cand_weight.T, preferred_element_type=jnp.float32)
    grad_tokens = inputs_grad.astype(jnp.bfloat16).reshape(2, SEQLEN, D)
    return grad_gate, grad_cand, grad_tokens
```

```python
import jax
import jax.numpy as jnp
from jax import lax
from jax.experimental import pallas as pl
from jax.experimental.pallas import tpu as pltpu
from jax.sharding import PartitionSpec as P


BF16 = jnp.bfloat16
F32 = jnp.float32
AXES = ("seq", "tp")
ZS, HS, CS, LS, YS = 4, 2, 2, 2, 4
TPS = LS * YS
CHUNKS = 8
LANES = 128


def move(block, dz=0, dh=0, dc=0, dl=0, dy=0):
    route = []
    for z in range(ZS):
        for h in range(HS):
            for c in range(CS):
                for l in range(LS):
                    for y in range(YS):
                        source = (((z * HS + h) * CS + c) * LS + l) * YS + y
                        target = ((((z + dz) % ZS * HS + (h + dh) % HS) * CS + (c + dc) % CS) * LS + (l + dl) % LS) * YS + (y + dy) % YS
                        route.append((source, target))
    return lax.ppermute(block, AXES, route)


def take(ref, rows):
    return jnp.concatenate([ref[q, rows, :] for q in range(ref.shape[0])], axis=1)


def put(ref, rows, value):
    for q in range(ref.shape[0]):
        ref[q, rows, :] = value[:, q * LANES : (q + 1) * LANES]


def forward_kernel(where, *refs):
    blocks = refs[:TPS]
    wg, wc, bias, score = refs[TPS : TPS + 4]
    keep_out, cand_out, score_out, sums_out, span_out, mine, theirs = refs[TPS + 4 : TPS + 11]
    acc_g, acc_c, scores = refs[TPS + 11 :]
    step = pl.program_id(0)
    core = where[TPS]
    half = mine.shape[2]
    for i in range(TPS):

        @pl.when(step == i)
        def _(i=i):
            block = blocks[i][...]
            g = jnp.dot(block, wg[...], preferred_element_type=F32)
            c = jnp.dot(block, wc[...], preferred_element_type=F32)
            for q in range(acc_g.shape[0]):
                lanes = slice(q * LANES, (q + 1) * LANES)
                if i == 0:
                    acc_g[q] = g[:, lanes]
                    acc_c[q] = c[:, lanes]
                    scores[q] = score[:, lanes]
                else:
                    acc_g[q] += g[:, lanes]
                    acc_c[q] += c[:, lanes]

            @pl.when(core == 0)
            def _():
                mine[0] = block[:, :half]
                theirs[0] = block[:, half:]

            @pl.when(core == 1)
            def _():
                mine[0] = block[:, half:]
                theirs[0] = block[:, :half]

    @pl.when(step == TPS - 1)
    def _():
        batch, steps, _, width = keep_out.shape
        length = steps * CHUNKS
        shift = bias[...]
        for b in range(batch):
            prod = jnp.ones((CHUNKS, width), F32)
            state = jnp.zeros((CHUNKS, width), F32)
            for j in range(steps):
                rows = pl.ds(b * length + j, CHUNKS, stride=steps)
                keep = jax.nn.sigmoid(take(acc_g, rows) + shift)
                cand = take(acc_c, rows)
                keep_out[b, j] = keep
                cand_out[b, j] = cand
                prod = prod * keep
                state = keep * state + (1.0 - keep) * cand
            back = jnp.zeros((CHUNKS, width), F32)
            for j in reversed(range(steps)):
                rows = pl.ds(b * length + j, CHUNKS, stride=steps)
                pull = take(scores, rows)
                score_out[b, j] = pull
                back = keep_out[b, j] * (pull + back)
            sums_out[b, 0] = prod
            sums_out[b, 1] = state
            sums_out[b, 2] = back
            whole = prod[0:1]
            ahead = state[0:1]
            for c in range(1, CHUNKS):
                whole = whole * prod[c : c + 1]
                ahead = prod[c : c + 1] * ahead + state[c : c + 1]
            behind = back[CHUNKS - 1 : CHUNKS]
            for c in reversed(range(CHUNKS - 1)):
                behind = back[c : c + 1] + prod[c : c + 1] * behind
            span_out[4 * b : 4 * b + 1] = whole
            span_out[4 * b + 1 : 4 * b + 2] = ahead
            span_out[4 * b + 2 : 4 * b + 3] = behind
            span_out[4 * b + 3 : 4 * b + 4] = jnp.zeros_like(whole)


def forward(where, blocks, wg, wc, bias, score, batch):
    rows, block = blocks[0].shape
    width = wg.shape[1]
    steps = rows // batch // CHUNKS
    tall = (batch, steps, CHUNKS, width)
    full = lambda shape: pl.BlockSpec(shape, lambda i, w: (0,) * len(shape))
    half = (1, rows, block // CS)
    return pl.pallas_call(
        forward_kernel,
        grid_spec=pltpu.PrefetchScalarGridSpec(
            num_scalar_prefetch=1,
            grid=(TPS,),
            in_specs=[full((rows, block))] * TPS
            + [pl.BlockSpec((block, width), lambda i, w: (w[i], 0))] * 2
            + [full((1, width)), full((rows, width))],
            out_specs=[full(tall), full(tall), full(tall), full((batch, 3, CHUNKS, width)), full((4 * batch, width))]
            + [pl.BlockSpec(half, lambda i, w: (w[i], 0, 0))] * 2,
            scratch_shapes=[pltpu.VMEM((width // LANES, rows, LANES), F32)] * 3,
        ),
        out_shape=[
            jax.ShapeDtypeStruct(tall, F32),
            jax.ShapeDtypeStruct(tall, F32),
            jax.ShapeDtypeStruct(tall, F32),
            jax.ShapeDtypeStruct((batch, 3, CHUNKS, width), F32),
            jax.ShapeDtypeStruct((4 * batch, width), F32),
            jax.ShapeDtypeStruct((TPS, *half[1:]), BF16),
            jax.ShapeDtypeStruct((TPS, *half[1:]), BF16),
        ],
        compiler_params=pltpu.CompilerParams(vmem_limit_bytes=40 << 20),
        name="project_and_scan",
    )(where, *blocks, wg, wc, bias, score)


def backward_kernel(place, keep_in, cand_in, sums, score, spans, deltas, before, tail, head, pres, cands):
    batch, steps, _, width = keep_in.shape
    length = steps * CHUNKS
    z, h, c = place[0], place[1], place[2]
    mine = (z * HS + h) * CS + c
    order = [(i // (HS * CS), i // CS % HS, i % CS) for i in range(ZS * HS * CS)]

    def span(i):
        oz, oh, oc = order[i]
        slot = (lax.rem(oz - z + ZS, ZS) * HS + lax.rem(oh + h, HS)) * CS + lax.rem(oc + c, CS)
        return spans[slot]

    for b in range(batch):
        into = jnp.zeros((1, width), F32)
        for i in range(len(order) - 1):
            s = span(i)
            into = jnp.where(i < mine, s[4 * b : 4 * b + 1] * into + s[4 * b + 1 : 4 * b + 2], into)
        back = jnp.zeros((1, width), F32)
        for i in reversed(range(1, len(order))):
            s = span(i)
            back = jnp.where(i > mine, s[4 * b : 4 * b + 1] * back + s[4 * b + 2 : 4 * b + 3], back)
        for k in range(CHUNKS):
            head[k : k + 1] = into
            into = sums[b, 0, k : k + 1] * into + sums[b, 1, k : k + 1]
        for k in reversed(range(CHUNKS)):
            tail[k : k + 1] = back
            back = sums[b, 0, k : k + 1] * back + sums[b, 2, k : k + 1]
        state = head[...]
        for j in range(steps):
            before[j] = state
            keep = keep_in[b, j]
            state = keep * state + (1.0 - keep) * cand_in[b, j]
        carry = tail[...]
        for j in reversed(range(steps)):
            rows = pl.ds(b * length + j, CHUNKS, stride=steps)
            keep = keep_in[b, j]
            adjoint = score[b, j] + carry
            fresh = adjoint * (1.0 - keep)
            put(pres, rows, fresh * keep * (before[j] - cand_in[b, j]))
            put(cands, rows, fresh)
            carry = keep * adjoint
    for q in range(width // LANES):
        deltas[:, q * LANES : (q + 1) * LANES] = pres[q].astype(BF16)
        deltas[:, width + q * LANES : width + (q + 1) * LANES] = cands[q].astype(BF16)


def backward(place, keep, cand, sums, score, spans):
    batch, steps, _, width = keep.shape
    rows = batch * steps * CHUNKS
    vmem = pl.BlockSpec(memory_space=pltpu.VMEM)
    return pl.pallas_call(
        backward_kernel,
        in_specs=[pl.BlockSpec(memory_space=pltpu.SMEM)] + [vmem] * 5,
        out_specs=vmem,
        out_shape=jax.ShapeDtypeStruct((rows, 2 * width), BF16),
        scratch_shapes=[
            pltpu.VMEM((steps, CHUNKS, width), F32),
            pltpu.VMEM((CHUNKS, width), F32),
            pltpu.VMEM((CHUNKS, width), F32),
            pltpu.VMEM((width // LANES, rows, LANES), F32),
            pltpu.VMEM((width // LANES, rows, LANES), F32),
        ],
        compiler_params=pltpu.CompilerParams(vmem_limit_bytes=40 << 20),
        name="scan_deltas",
    )(place, keep, cand, sums, score, spans)


def weights_kernel(pick, own, other, d_own, d_other, out):
    contract = (((0,), (0,)), ((), ()))
    total = lax.dot_general(own[0], d_own[...], contract, preferred_element_type=F32)
    total = total + lax.dot_general(other[0], d_other[...], contract, preferred_element_type=F32)
    out[0] = total.astype(BF16)


def weights(pick, own, other, d_own, d_other):
    count = pick.shape[0]
    rows, half = own.shape[1:]
    wide = d_own.shape[1]
    full = pl.BlockSpec((rows, wide), lambda i, w: (0, 0))
    return pl.pallas_call(
        weights_kernel,
        grid_spec=pltpu.PrefetchScalarGridSpec(
            num_scalar_prefetch=1,
            grid=(count,),
            in_specs=[pl.BlockSpec((1, rows, half), lambda i, w: (w[i], 0, 0))] * 2 + [full] * 2,
            out_specs=pl.BlockSpec((1, half, wide), lambda i, w: (i, 0, 0)),
        ),
        out_shape=jax.ShapeDtypeStruct((count, half, wide), BF16),
        compiler_params=pltpu.CompilerParams(vmem_limit_bytes=40 << 20),
        name="weight_grads",
    )(pick, own, other, d_own, d_other)


def inputs_kernel(pick, deltas, wg, wc, out):
    contract = (((1,), (1,)), ((), ()))
    width = wg.shape[1]
    total = lax.dot_general(deltas[:, :width], wg[...], contract, preferred_element_type=F32)
    total = total + lax.dot_general(deltas[:, width:], wc[...], contract, preferred_element_type=F32)
    out[0] = total.astype(BF16)


def inputs(pick, deltas, wg, wc, block):
    count = pick.shape[0]
    rows, wide = deltas.shape
    width = wg.shape[1]
    return pl.pallas_call(
        inputs_kernel,
        grid_spec=pltpu.PrefetchScalarGridSpec(
            num_scalar_prefetch=1,
            grid=(count,),
            in_specs=[pl.BlockSpec((rows, wide), lambda i, w: (0, 0))]
            + [pl.BlockSpec((block, width), lambda i, w: (w[i], 0))] * 2,
            out_specs=pl.BlockSpec((1, rows, block), lambda i, w: (i, 0, 0)),
        ),
        out_shape=jax.ShapeDtypeStruct((count, rows, block), BF16),
        compiler_params=pltpu.CompilerParams(vmem_limit_bytes=40 << 20),
        name="input_grads",
    )(pick, deltas, wg, wc)


def plus(*parts):
    total = parts[0].astype(F32)
    for part in parts[1:]:
        total = total + part.astype(F32)
    return total


def shards(tokens, gate_weight, cand_weight, forget_bias, readout, advantage):
    batch, count, block = tokens.shape
    width = gate_weight.shape[1]
    rows = batch * count
    seq = lax.axis_index("seq")
    tp = lax.axis_index("tp")
    z, h, c = seq // (HS * CS), seq // CS % HS, seq % CS
    l, y = tp // YS, tp % YS

    own = tokens.reshape(rows, block)
    across = move(own, dl=1)
    lower = move(own, dy=1)
    upper = move(own, dy=-1)
    part = rows // 2
    far = jnp.concatenate([move(lower[:part], dy=1), move(upper[part:], dy=-1)], axis=0)
    across_lower = move(across, dy=1)
    across_upper = move(across, dy=-1)
    across_far = move(far, dl=1)
    at = lambda dl, dy: (l + dl) % LS * YS + (y + dy) % YS
    blocks = [own, across, lower, upper, across_lower, across_upper, far, across_far]
    where = jnp.stack([at(0, 0), at(1, 0), at(0, 3), at(0, 1), at(1, 3), at(1, 1), at(0, 2), at(1, 2), c]).astype(jnp.int32)
    score = ((advantage.astype(F32) * 0.25)[:, :, None] * readout.astype(F32)).reshape(rows, width)
    keep, cand, pull, sums, span, mine, theirs = forward(where, blocks, gate_weight, cand_weight, forget_bias.reshape(1, width), score, batch)

    spans = jnp.stack([span, move(span, dc=1)])
    spans = jnp.concatenate([spans, move(spans, dh=1)])
    spans = jnp.concatenate([spans, move(spans, dz=-1), move(spans, dz=2), move(spans, dz=1)])
    others = move(theirs, dc=1)
    place = jnp.stack([z, h, c]).astype(jnp.int32)
    deltas = backward(place, keep, cand, sums, pull, spans)

    their_deltas = move(deltas, dc=1)
    chip = lambda dz, dh: (z + dz) % ZS * HS + (h + dh) % HS
    pick = lambda *items: jnp.stack(items).astype(jnp.int32)
    opposite = weights(pick(chip(2, 0), chip(2, 1)), mine, others, deltas, their_deltas)
    met_lower = move(opposite[:, :, :width], dz=1)
    met_upper = move(opposite[:, :, width:], dz=-1)
    nearby = weights(pick(chip(1, 0), chip(1, 1), chip(3, 0), chip(3, 1), chip(0, 1), chip(0, 0)), mine, others, deltas, their_deltas)
    to_upper = jnp.concatenate([plus(nearby[0:2, :, :width], met_lower).astype(BF16), nearby[0:2, :, width:]], axis=2)
    to_lower = jnp.concatenate([nearby[2:4, :, :width], plus(nearby[2:4, :, width:], met_upper).astype(BF16)], axis=2)
    from_lower = move(to_upper, dz=1)
    from_upper = move(to_lower, dz=-1)
    to_pair = plus(nearby[4], from_lower[1], from_upper[1]).astype(BF16)
    from_pair = move(to_pair, dh=1)
    both = plus(nearby[5], from_lower[0], from_upper[0], from_pair)
    grad_gate = both[:, :width]
    grad_cand = both[:, width:]

    t_far = inputs(pick(at(0, 2), at(1, 2)), deltas, gate_weight, cand_weight, block)
    t_lower = move(t_far[0], dy=1)
    t_upper = move(t_far[1], dy=-1)
    t_near = inputs(pick(at(0, 1), at(1, 1), at(0, 3), at(1, 3), at(1, 0), at(0, 0)), deltas, gate_weight, cand_weight, block)
    u_lower = move(jnp.stack([plus(t_near[0], t_lower).astype(BF16), t_near[1]]), dy=1)
    u_upper = move(jnp.stack([t_near[2], plus(t_near[3], t_upper).astype(BF16)]), dy=-1)
    t_pair = move(plus(t_near[4], u_lower[1], u_upper[1]).astype(BF16), dl=1)
    grad_tokens = plus(t_near[5], u_lower[0], u_upper[0], t_pair).astype(BF16).reshape(batch, count, block)
    return (grad_gate, grad_cand, grad_tokens)


def solution(mesh):
    in_specs = (
        P(None, "seq", "tp"),
        P(None, "tp"),
        P(None, "tp"),
        P("tp"),
        P(None, "seq", "tp"),
        P(None, "seq"),
    )
    out_specs = (P("seq", "tp"), P("seq", "tp"), P(None, "seq", "tp"))
    return jax.shard_map(shards, mesh=mesh, in_specs=in_specs, out_specs=out_specs, check_vma=False)
```

```python
import functools

import jax
import jax.numpy as jnp
from jax import lax
from jax.experimental import pallas as pl
from jax.experimental.pallas import tpu as pltpu
from jax.sharding import PartitionSpec as P


BF16 = jnp.bfloat16
F32 = jnp.float32
AXES = ("seq", "tp")
ZS, HS, CS, LS, YS = 4, 2, 2, 2, 4
TPS = LS * YS
CHUNKS = 8
LANES = 128
EARLY = 5
SPLIT = 640
BLOCKS = ((0, 0), (0, 3), (0, 1), (1, 0), (0, 2), (1, 3), (1, 1), (1, 2))
LIMIT = 8 << 20


def move(block, dz=0, dh=0, dc=0, dl=0, dy=0):
    route = []
    for z in range(ZS):
        for h in range(HS):
            for c in range(CS):
                for l in range(LS):
                    for y in range(YS):
                        source = (((z * HS + h) * CS + c) * LS + l) * YS + y
                        target = ((((z + dz) % ZS * HS + (h + dh) % HS) * CS + (c + dc) % CS) * LS + (l + dl) % LS) * YS + (y + dy) % YS
                        route.append((source, target))
    return lax.ppermute(block, AXES, route)


def take(ref, rows):
    return jnp.concatenate([ref[q, rows, :] for q in range(ref.shape[0])], axis=1)


def put(ref, rows, value):
    for q in range(ref.shape[0]):
        ref[q, rows, :] = value[:, q * LANES : (q + 1) * LANES]


def feature(coords, dl, dy):
    return lax.rem(coords[3] + dl, LS) * YS + lax.rem(coords[4] + dy, YS)


def slot(coords, dz, dh):
    want = lax.rem(coords[0] + dz, ZS) * HS + lax.rem(coords[1] + dh, HS)
    dl = lax.rem(lax.div(want, YS) + LS - coords[3], LS)
    return dl * YS + lax.rem(lax.rem(want, YS) + YS - coords[4], YS)


def joined(blocks):
    return jnp.concatenate([ref[...] for ref in blocks], axis=1)


def fetch(weights, block, rows, slot, sems):
    size, wide = rows.shape[1:]
    copies = []
    for side, w in enumerate(weights):
        source = w.at[pl.ds(pl.multiple_of(block * size, size), size), :]
        target = rows.at[slot, :, pl.ds(side * (wide // 2), wide // 2)]
        copies.append(pltpu.make_async_copy(source, target, sems.at[slot, side]))
    for copy in copies:
        copy.start()
    return copies


def early_kernel(coords, *refs):
    blocks = refs[:EARLY]
    wg, wc, acc, rest, rows, sems, rest_sems = refs[EARLY:]
    size, wide = rows.shape[1:]
    copies = [fetch((wg, wc), feature(coords, *BLOCKS[i]), rows, i, sems) for i in range(EARLY)]
    rest_copies = [fetch((wg, wc), feature(coords, *BLOCKS[EARLY + i]), rest, i, rest_sems) for i in range(TPS - EARLY)]
    for pair in copies:
        for copy in pair:
            copy.wait()
    acc[...] = jnp.dot(joined(blocks), rows[...].reshape(EARLY * size, wide), preferred_element_type=F32)
    for pair in rest_copies:
        for copy in pair:
            copy.wait()


def late_kernel(*refs):
    count = TPS - EARLY
    rows, bias, score, start = refs[count : count + 4]
    keep_out, cand_out, score_out, sums_out, span_out = refs[count + 4 : count + 9]
    acc_g, acc_c, scores = refs[count + 9 :]
    size, wide = rows.shape[1:]
    spread = rows[...].reshape(count * size, wide)
    both = start[...] + jnp.dot(joined(refs[:count]), spread, preferred_element_type=F32)
    g, c = both[:, : wide // 2], both[:, wide // 2 :]
    for q in range(scores.shape[0]):
        lanes = slice(q * LANES, (q + 1) * LANES)
        acc_g[q] = g[:, lanes]
        acc_c[q] = c[:, lanes]
        scores[q] = score[:, lanes]
    batch, steps, _, width = keep_out.shape
    length = steps * CHUNKS
    shift = bias[...]
    for b in range(batch):
        prod = jnp.ones((CHUNKS, width), F32)
        state = jnp.zeros((CHUNKS, width), F32)
        for j in range(steps):
            rows = pl.ds(b * length + j, CHUNKS, stride=steps)
            keep = jax.nn.sigmoid(take(acc_g, rows) + shift)
            cand = take(acc_c, rows)
            keep_out[b, j] = keep
            cand_out[b, j] = cand
            prod = prod * keep
            state = keep * state + (1.0 - keep) * cand
        back = jnp.zeros((CHUNKS, width), F32)
        for j in reversed(range(steps)):
            rows = pl.ds(b * length + j, CHUNKS, stride=steps)
            pull = take(scores, rows)
            score_out[b, j] = pull
            back = keep_out[b, j] * (pull + back)
        sums_out[b, 0] = prod
        sums_out[b, 1] = state
        sums_out[b, 2] = back
        whole = prod[0:1]
        ahead = state[0:1]
        for c in range(1, CHUNKS):
            whole = whole * prod[c : c + 1]
            ahead = prod[c : c + 1] * ahead + state[c : c + 1]
        behind = back[CHUNKS - 1 : CHUNKS]
        for c in reversed(range(CHUNKS - 1)):
            behind = back[c : c + 1] + prod[c : c + 1] * behind
        span_out[4 * b : 4 * b + 1] = whole
        span_out[4 * b + 1 : 4 * b + 2] = ahead
        span_out[4 * b + 2 : 4 * b + 3] = behind
        span_out[4 * b + 3 : 4 * b + 4] = jnp.zeros_like(whole)


def cost(flops):
    return pl.CostEstimate(flops=3 * flops, transcendentals=0, bytes_accessed=0)


def local(kernel, inputs, out_shape, scratch=(), flops=0, scalars=1, remote=0):
    vmem = pl.BlockSpec(memory_space=pltpu.VMEM)
    return pl.pallas_call(
        kernel,
        in_specs=[pl.BlockSpec(memory_space=pltpu.SMEM)] * scalars + [vmem] * (len(inputs) - scalars - remote) + [pl.BlockSpec(memory_space=pltpu.HBM)] * remote,
        out_specs=jax.tree.map(lambda _: vmem, out_shape),
        out_shape=out_shape,
        scratch_shapes=list(scratch),
        compiler_params=pltpu.CompilerParams(vmem_limit_bytes=LIMIT),
        cost_estimate=cost(flops),
    )(*inputs)


def early(coords, blocks, wg, wc):
    count, (rows, block) = len(blocks), blocks[0].shape
    wide = 2 * wg.shape[1]
    return local(
        early_kernel,
        (coords, *blocks, wg, wc),
        [jax.ShapeDtypeStruct((rows, wide), F32), jax.ShapeDtypeStruct((TPS - count, block, wide), BF16)],
        [pltpu.VMEM((count, block, wide), BF16), pltpu.SemaphoreType.DMA((count, 2)), pltpu.SemaphoreType.DMA((TPS - count, 2))],
        flops=2 * rows * block * wide * count,
        remote=2,
    )


def late(blocks, spread, bias, score, start, batch):
    rows, block = blocks[0].shape
    width = bias.shape[1]
    tall = jax.ShapeDtypeStruct((batch, rows // batch // CHUNKS, CHUNKS, width), F32)
    sums = jax.ShapeDtypeStruct((batch, 3, CHUNKS, width), F32)
    span = jax.ShapeDtypeStruct((4 * batch, width), F32)
    return local(
        late_kernel,
        (*blocks, spread, bias, score, start),
        [tall, tall, tall, sums, span],
        [pltpu.VMEM((width // LANES, rows, LANES), F32)] * 3,
        flops=4 * rows * block * width * len(blocks),
        scalars=0,
    )


def arrange_kernel(coords, *refs):
    mine, theirs = refs[TPS:]
    half = mine.shape[2]
    for i in range(TPS):
        low, high = refs[i][:, :half], refs[i][:, half:]
        mine[i] = jnp.where(coords[2] == 0, low, high)
        theirs[i] = jnp.where(coords[2] == 0, high, low)


def arrange(coords, blocks):
    rows, block = blocks[0].shape
    half = jax.ShapeDtypeStruct((TPS, rows, block // CS), BF16)
    return local(arrange_kernel, (coords, *blocks), [half, half], flops=1 << 27)


def backward_kernel(place, keep_in, cand_in, sums, score, spans, deltas, before, tail, head, pres, cands):
    batch, steps, _, width = keep_in.shape
    length = steps * CHUNKS
    z, h, c = place[0], place[1], place[2]
    mine = (z * HS + h) * CS + c
    order = [(i // (HS * CS), i // CS % HS, i % CS) for i in range(ZS * HS * CS)]

    def span(i):
        oz, oh, oc = order[i]
        slot = (lax.rem(oz - z + ZS, ZS) * HS + lax.rem(oh + h, HS)) * CS + lax.rem(oc + c, CS)
        return spans[slot]

    for b in range(batch):
        into = jnp.zeros((1, width), F32)
        for i in range(len(order) - 1):
            s = span(i)
            into = jnp.where(i < mine, s[4 * b : 4 * b + 1] * into + s[4 * b + 1 : 4 * b + 2], into)
        back = jnp.zeros((1, width), F32)
        for i in reversed(range(1, len(order))):
            s = span(i)
            back = jnp.where(i > mine, s[4 * b : 4 * b + 1] * back + s[4 * b + 2 : 4 * b + 3], back)
        for k in range(CHUNKS):
            head[k : k + 1] = into
            into = sums[b, 0, k : k + 1] * into + sums[b, 1, k : k + 1]
        for k in reversed(range(CHUNKS)):
            tail[k : k + 1] = back
            back = sums[b, 0, k : k + 1] * back + sums[b, 2, k : k + 1]
        state = head[...]
        for j in range(steps):
            before[j] = state
            keep = keep_in[b, j]
            state = keep * state + (1.0 - keep) * cand_in[b, j]
        carry = tail[...]
        for j in reversed(range(steps)):
            rows = pl.ds(b * length + j, CHUNKS, stride=steps)
            keep = keep_in[b, j]
            adjoint = score[b, j] + carry
            fresh = adjoint * (1.0 - keep)
            put(pres, rows, fresh * keep * (before[j] - cand_in[b, j]))
            put(cands, rows, fresh)
            carry = keep * adjoint
    for q in range(width // LANES):
        deltas[:, q * LANES : (q + 1) * LANES] = pres[q].astype(BF16)
        deltas[:, width + q * LANES : width + (q + 1) * LANES] = cands[q].astype(BF16)


def backward(place, keep, cand, sums, score, spans):
    batch, steps, _, width = keep.shape
    rows = batch * steps * CHUNKS
    return local(
        backward_kernel,
        (place, keep, cand, sums, score, spans),
        jax.ShapeDtypeStruct((rows, 2 * width), BF16),
        [pltpu.VMEM((steps, CHUNKS, width), F32)]
        + [pltpu.VMEM((CHUNKS, width), F32)] * 2
        + [pltpu.VMEM((width // LANES, rows, LANES), F32)] * 2,
        flops=1 << 28,
    )


def weights_kernel(coords, own, other, d_own, d_other, *outs, spots, low, high):
    half = own.shape[2]
    slots = [slot(coords, *spot) for spot in spots]
    lhs = jnp.concatenate([jnp.concatenate([own[i], other[i]], axis=0) for i in slots], axis=1)
    rhs = jnp.concatenate([d_own[:, low:high], d_other[:, low:high]], axis=0)
    total = lax.dot_general(lhs, rhs, (((0,), (0,)), ((), ())), preferred_element_type=F32)
    for i, out in enumerate(outs):
        out[...] = total[i * half : (i + 1) * half].astype(BF16)


def weights(coords, spots, own, other, d_own, d_other, low, high):
    count = len(spots)
    rows, half = own.shape[1:]
    return local(
        functools.partial(weights_kernel, spots=spots, low=low, high=high),
        (coords, own, other, d_own, d_other),
        [jax.ShapeDtypeStruct((half, high - low), BF16)] * count,
        flops=4 * rows * half * count * (high - low),
    )


def rows_kernel(coords, wg, wc, rows, sems):
    copies = [fetch((wg, wc), feature(coords, *BLOCKS[i]), rows, i, sems) for i in range(TPS)]
    for pair in copies:
        for copy in pair:
            copy.wait()


def weight_rows(coords, wg, wc, block):
    return local(
        rows_kernel,
        (coords, wg, wc),
        jax.ShapeDtypeStruct((TPS, block, 2 * wg.shape[1]), BF16),
        [pltpu.SemaphoreType.DMA((TPS, 2))],
        flops=1 << 27,
        remote=2,
    )


def inputs_kernel(deltas, rows, *outs, spots):
    for spot, out in zip(spots, outs, strict=True):
        weight = rows[BLOCKS.index(spot)]
        total = lax.dot_general(deltas[...], weight, (((1,), (1,)), ((), ())), preferred_element_type=F32)
        out[...] = total.astype(BF16)


def inputs(spots, deltas, rows):
    count, wide = deltas.shape
    block = rows.shape[1]
    return local(
        functools.partial(inputs_kernel, spots=spots),
        (deltas, rows),
        [jax.ShapeDtypeStruct((count, block), BF16)] * len(spots),
        flops=2 * count * wide * block * len(spots),
        scalars=0,
    )


def plus(*parts):
    total = parts[0].astype(F32)
    for part in parts[1:]:
        total = total + part.astype(F32)
    return total


def layer(tokens, gate_weight, cand_weight, forget_bias, readout, advantage):
    batch, count, block = tokens.shape
    width = gate_weight.shape[1]
    rows = batch * count
    seq = lax.axis_index("seq")
    tp = lax.axis_index("tp")
    places = [lax.div(seq, HS * CS), lax.rem(lax.div(seq, CS), HS), lax.rem(seq, CS), lax.div(tp, YS), lax.rem(tp, YS)]
    coords = jnp.stack(places).astype(jnp.int32)
    gate_weight = pltpu.with_memory_space_constraint(gate_weight, pltpu.HBM)
    cand_weight = pltpu.with_memory_space_constraint(cand_weight, pltpu.HBM)

    own = tokens.reshape(rows, block)
    part = rows // 2
    lower = move(own, dy=1)
    upper = move(own, dy=-1)
    across = move(own, dl=1)
    far = jnp.concatenate([move(lower[:part], dy=1), move(upper[part:], dy=-1)], axis=0)
    across_lower = move(across, dy=1)
    across_upper = move(across, dy=-1)
    across_far = move(far, dl=1)
    blocks = [own, lower, upper, across, far, across_lower, across_upper, across_far]
    score = ((advantage.astype(F32) * 0.25)[:, :, None] * readout.astype(F32)).reshape(rows, width)
    start, spread = early(coords, blocks[:EARLY], gate_weight, cand_weight)
    keep, cand, pull, sums, span = late(blocks[EARLY:], spread, forget_bias.reshape(1, width), score, start, batch)

    spans = jnp.stack([span, move(span, dc=1)])
    ordered = [own, upper, far, lower, across, across_upper, across_far, across_lower]
    mine, theirs = arrange(coords, ordered)
    weight_block = weight_rows(coords, gate_weight, cand_weight, block)
    others = move(theirs, dc=1)
    spans = jnp.concatenate([spans, move(spans, dh=1)])
    spans = jnp.concatenate([spans, move(spans, dz=-1), move(spans, dz=2), move(spans, dz=1)])
    deltas = backward(coords, keep, cand, sums, pull, spans)

    their_deltas = move(deltas, dc=1)
    t_grads = lambda *spots: inputs(spots, deltas, weight_block)
    t_far = t_grads((0, 2), (1, 2))
    t_lower = move(t_far[0], dy=1)
    t_upper = move(t_far[1], dy=-1)

    grads = lambda spots, low, high: weights(coords, spots, mine, others, deltas, their_deltas, low, high)
    wide = 2 * width
    opposite = grads([(2, 0), (2, 1)], 0, SPLIT)
    met_lower = move(opposite[0], dz=1)
    met_upper = move(opposite[1], dz=-1)
    pair_out = move(jnp.stack(grads([(0, 1), (1, 1), (2, 1), (3, 1)], SPLIT, wide)), dh=1)
    t_near = t_grads((0, 1), (1, 1), (0, 3), (1, 3))
    nearby = grads([(1, 0), (1, 1), (3, 0), (3, 1)], 0, SPLIT)
    t_near += t_grads((1, 0), (0, 0))
    nearby += grads([(0, 1), (0, 0)], 0, SPLIT)
    pair_own = grads([(0, 0), (1, 0), (2, 0), (3, 0)], SPLIT, wide)

    u_lower = move(jnp.stack([plus(t_near[0], t_lower).astype(BF16), t_near[1]]), dy=1)
    u_upper = move(jnp.stack([t_near[2], plus(t_near[3], t_upper).astype(BF16)]), dy=-1)
    from_lower = move(jnp.stack([plus(nearby[0], met_lower).astype(BF16), nearby[1]]), dz=1)
    from_upper = move(jnp.stack([nearby[2], plus(nearby[3], met_upper).astype(BF16)]), dz=-1)
    t_pair = move(plus(t_near[4], u_lower[1], u_upper[1]).astype(BF16), dl=1)
    from_pair = move(plus(nearby[4], from_lower[1], from_upper[1]).astype(BF16), dh=1)
    pair = [plus(pair_own[i], pair_out[i]) for i in range(ZS)]
    pair_in = [move(pair[i].astype(BF16), dz=i) for i in range(1, ZS)]
    left = plus(nearby[5], from_lower[0], from_upper[0], from_pair)
    right = plus(pair[0], *pair_in)
    grad_gate = left[:, :width]
    grad_cand = jnp.concatenate([left[:, width:], right], axis=1)
    grad_tokens = plus(t_near[5], u_lower[0], u_upper[0], t_pair).astype(BF16).reshape(batch, count, block)
    return (grad_gate, grad_cand, grad_tokens)


def solution(mesh):
    in_specs = (
        P(None, "seq", "tp"),
        P(None, "tp"),
        P(None, "tp"),
        P("tp"),
        P(None, "seq", "tp"),
        P(None, "seq"),
    )
    out_specs = (P("seq", "tp"), P("seq", "tp"), P(None, "seq", "tp"))
    return jax.shard_map(layer, mesh=mesh, in_specs=in_specs, out_specs=out_specs, check_vma=False)
```
